32 devices in a mesh: seq: 8 (over z, x), tp: 4 (over y, core).
Axes of the slice: x: 2, y: 2, z: 4, core: 2. Of those that a mesh axis runs over, the one named last changes fastest.
Arguments:
- tokens: bfloat16 [1024, 6144], P('seq', 'tp'), may hold values from -6 to 6
- router_weight: bfloat16 [6144, 8], P('tp'), may hold values from -0.15625 to 0.15625
- expert_ids: int32 [1024, 2], P('seq'), may hold values from 0 to 7, all different within a row; in each aligned block of 128 rows (0 to 127, 128 to 255, ...) at most 56 rows name the same one
- gate_weight: bfloat16 [8, 6144, 8192], P('seq', None, 'tp'), may hold values from -0.078125 to 0.078125
- up_weight: bfloat16 [8, 6144, 8192], P('seq', None, 'tp'), may hold values from -0.078125 to 0.078125
- down_weight: bfloat16 [8, 8192, 6144], P('seq', 'tp'), may hold values from -0.0625 to 0.0625
Outputs:
- mixed: bfloat16 [1024, 6144], P('seq', 'tp')
The draws below stay inside these ranges and needn't reach their ends.
Inputs may be any that keep to these rules, and one draw needn't show every extreme that they name: `expert_ids`: each row names 2 different experts. In each aligned block of 128 rows (the tokens of one sequence group) no expert is named more than 56 times, a bound that some block reaches.
All inputs are finite; a program needn't handle non-finite values.
Results may differ from the reference program's by a relative error of at most 0.014.
Values may be sent and summed in bfloat16 or wider, within the bound.
A program may use at most 128 MiB of HBM per device.

```python
import math
import jax
import jax.numpy as jnp
import numpy as np
from jax import lax

D = 6144
EXPERTS = 8
FF = 8192
TOP = 2
TOK_SEQ = 128
CAP = 56
SPLIT = 1
TOKENS = 1024
N_SEQ = 8
N_TP = 4


def steps_of(own_key, extent, shards, least, top_value):
    gain, own = 1.0, jax.random.fold_in(own_key, 6)
    for dim, parts in shards:
        steps = jnp.exp(jax.random.uniform(jax.random.fold_in(own, dim), (parts,), jnp.float32, least / len(shards), top_value / len(shards)))
        gain = gain * jnp.repeat(steps, extent[dim] // parts).reshape([-1 if axis == dim else 1 for axis in range(len(extent))])
    return gain


def shared_out(stream_key, own, number, rows, amount, top, limit, lean):
    order = jax.random.permutation(stream_key, amount)
    heavy_load, usual = load_shares(amount, rows * top, limit, lean, True), load_shares(amount, rows * top, limit, lean, False)
    places = jnp.arange(amount)

    def named(sizes, rotation):
        used = int((sizes > 0).sum())
        fixed = max(1, used // 4)
        passed = fixed + (places - fixed + rotation * (used - fixed)) % max(1, amount - fixed)
        return jnp.zeros((amount,), jnp.int32).at[order[jnp.where(places < fixed, places, passed)]].set(jnp.asarray(sizes, jnp.int32))

    sizes = jnp.where(number % 4 == 0, named(heavy_load, number // 4), named(usual, number - number // 4 - 1))
    mixed = jax.random.permutation(jax.random.fold_in(own, 3), amount)
    giver, taker = mixed[0:amount // 2 * 2:2], mixed[1:amount // 2 * 2:2]
    margin = jnp.minimum(sizes[giver] - 1, limit - sizes[taker]) // 2
    margin = jnp.where((giver == order[0]) | (taker == order[0]) | (sizes[taker] == 0), 0, jnp.maximum(margin, 0))
    passed = jax.random.randint(jax.random.fold_in(own, 4), (amount // 2,), 0, 1 << 20) % (margin + 1)
    sizes = sizes.at[giver].add(-passed).at[taker].add(passed)
    labels = jnp.searchsorted(jnp.cumsum(sizes), jnp.arange(rows * top), side="right").astype(jnp.int32)
    table = labels.reshape(top, rows).T
    table = table[jax.random.permutation(jax.random.fold_in(own, 1), rows)]
    rotation = jax.random.randint(jax.random.fold_in(own, 2), (rows, 1), 0, top)
    return jnp.take_along_axis(table, (jnp.arange(top)[None, :] + rotation) % top, axis=1)


def load_shares(number_of, total, reach, slope, full):
    loads = [(1 << 20) // math.isqrt(rank ** slope) + 1 for rank in range(1, number_of + 1)]
    largest = reach if full else min(reach, max(-(-total // number_of), total * loads[0] // sum(loads)))
    least = 1 if total - largest >= number_of - 1 else 0
    counts, surplus = [largest] + [least] * (number_of - 1), total - largest - least * (number_of - 1)
    while surplus > 0:
        movable = [i for i in range(1, number_of) if counts[i] < largest] or [i for i in range(1, number_of) if counts[i] < reach]
        whole, left = sum([loads[i] for i in movable]), surplus
        for i in movable:
            extra = min(reach - counts[i], max(1, left * loads[i] // whole), surplus)
            counts[i] = counts[i] + extra
            surplus = surplus - extra
    return np.array(counts)


def scatter_about(key, shape, spread, bound, pieces=(), held_as=jnp.bfloat16):
    entries = jax.random.normal(key, shape, jnp.float32) * spread
    if len(pieces) > 0:
        entries = steps_of(key, shape, pieces, -0.22, 0.18) * entries
    return jnp.clip(entries, min=-bound, max=bound).astype(held_as)


def setup_inputs(seed: int = 0) -> dict:
    streams_of = jax.random.split(jax.random.key(seed), 7)
    tokens = scatter_about(streams_of[0], (TOKENS, D), 1.0, 6.0, ((0, 8), (1, 4)))
    router_weight = scatter_about(streams_of[1], (D, EXPERTS), (D // 4) ** -0.5, 0.15625, ((0, 4),))
    expert_ids_keys = jax.random.split(jax.random.fold_in(streams_of[2], 1), TOKENS // TOK_SEQ)
    expert_ids_turns = jax.random.permutation(jax.random.fold_in(streams_of[2], 3), TOKENS // TOK_SEQ)
    expert_ids = jax.vmap(lambda own, number: shared_out(jax.random.fold_in(streams_of[2], 2), own, number, TOK_SEQ, EXPERTS, TOP, CAP, 2))(expert_ids_keys, expert_ids_turns).reshape((TOKENS, TOP))
    gate_weight = scatter_about(streams_of[3], (N_SEQ, D, FF // SPLIT), D ** -0.5, 0.078125, ((0, 8), (2, 4)))
    up_weight = scatter_about(streams_of[4], (N_SEQ, D, FF // SPLIT), D ** -0.5, 0.078125, ((0, 8), (2, 4)))
    down_weight = scatter_about(streams_of[5], (N_SEQ, FF // SPLIT, D), FF ** -0.5, 0.0625, ((0, 8), (1, 4)))
    return dict(tokens=tokens, router_weight=router_weight, expert_ids=expert_ids, gate_weight=gate_weight, up_weight=up_weight, down_weight=down_weight)


def reference(tokens, router_weight, expert_ids, gate_weight, up_weight, down_weight):
    halves = N_SEQ // EXPERTS
    block = FF // (halves * N_TP)
    logits = jnp.dot(tokens, router_weight, preferred_element_type=jnp.float32)
    chosen = expert_ids[:, :, None] == jnp.arange(EXPERTS, dtype=jnp.int32)[None, None, :]
    picked = jnp.sum(jnp.where(chosen, logits[:, None, :], jnp.float32(0.0)), axis=2)
    gates = jax.nn.sigmoid(picked - picked[:, ::-1])
    grouped = expert_ids.reshape(N_SEQ, TOK_SEQ * TOP)
    onehot = (grouped[:, :, None] == jnp.arange(EXPERTS, dtype=jnp.int32)[None, None, :]).astype(jnp.int32)
    before = jnp.cumsum(onehot, axis=1) - onehot
    slots = jnp.sum(before * onehot, axis=2).astype(jnp.int32)
    group_index = jnp.broadcast_to(jnp.arange(N_SEQ, dtype=jnp.int32)[:, None], grouped.shape)
    token_index = (group_index * TOK_SEQ + jnp.arange(TOK_SEQ * TOP, dtype=jnp.int32)[None, :] // TOP).astype(jnp.int32)
    table = jnp.full((EXPERTS, N_SEQ, CAP), TOKENS, jnp.int32).at[grouped, group_index, slots].set(token_index)
    padded = jnp.concatenate([tokens, jnp.zeros((1, D), tokens.dtype)], axis=0)

    def one_expert(expert):
        selected = padded[table[expert].reshape(-1)]
        total = jnp.zeros((N_SEQ * CAP, D), jnp.float32)
        for portion in range(halves):
            slab_index = expert * halves + portion
            gate_slab = gate_weight[slab_index]
            up_slab = up_weight[slab_index]
            down_slab = down_weight[slab_index]
            for shard in range(N_TP):
                low = shard * block
                gate = jnp.dot(selected, gate_slab[:, low:low + block], preferred_element_type=jnp.float32)
                up = jnp.dot(selected, up_slab[:, low:low + block], preferred_element_type=jnp.float32)
                hidden = (jax.nn.silu(gate) * up).astype(jnp.bfloat16)
                product = jnp.dot(hidden, down_slab[low:low + block, :], preferred_element_type=jnp.float32)
                rounded = lax.optimization_barrier(product.astype(jnp.bfloat16))
                total = total + rounded.astype(jnp.float32)
        return total

    outputs = lax.map(one_expert, jnp.arange(EXPERTS, dtype=jnp.int32))
    where_from = (grouped * (N_SEQ * CAP) + group_index * CAP + slots).astype(jnp.int32)
    gathered = outputs.reshape(EXPERTS * N_SEQ * CAP, D)[where_from.reshape(-1)].reshape(TOKENS, TOP, D)
    mixed = jnp.sum(gathered * gates[:, :, None], axis=1)
    return mixed.astype(jnp.bfloat16)
```

```python
import functools

import jax
import jax.numpy as jnp
from jax import lax
from jax.experimental import pallas as pl
from jax.experimental.pallas import tpu as pltpu
from jax.sharding import PartitionSpec as P

CAP = 56
CORES = 2


def slot_numbers(expert_ids, experts):
    flat_ids = expert_ids.reshape(-1)
    onehot = (flat_ids[:, None] == jnp.arange(experts, dtype=jnp.int32)[None, :]).astype(jnp.int32)
    before = jnp.cumsum(onehot, axis=0) - onehot
    return (flat_ids, jnp.sum(before * onehot, axis=1))


def flip(index, mask):
    bit = 1
    while bit <= mask:
        if mask & bit:
            index = index + (1 - 2 * ((index // bit) % 2)) * bit
        bit *= 2
    return index


def interleaved(seq):
    far, near = list(range(seq // 2, seq)), list(range(1, seq // 2))
    order = []
    while far or near:
        order += far[:1] + near[:1]
        far, near = far[1:], near[1:]
    return order


def remote(src, dst, send, recv, seq, tp):
    return pltpu.make_async_remote_copy(
        src_ref=src,
        dst_ref=dst,
        send_sem=send,
        recv_sem=recv,
        device_id={"seq": seq, "tp": tp},
        device_id_type=pl.DeviceIdType.MESH,
    )


def greet(seq, tp, s, t):
    barrier = pltpu.get_barrier_semaphore()
    for off in range(1, seq):
        pl.semaphore_signal(
            barrier, inc=1, device_id={"seq": flip(s, off), "tp": t}, device_id_type=pl.DeviceIdType.MESH
        )
    for off in range(1, tp):
        pl.semaphore_signal(
            barrier, inc=1, device_id={"seq": s, "tp": (t + off) % tp}, device_id_type=pl.DeviceIdType.MESH
        )
    pl.semaphore_wait(barrier, seq - 1 + tp - 1)


def dispatch_kernel(
    seq, tp, x_ref, part_ref, out_ref, logits_ref,
    local_sem, a_send, a_recv, d_send, d_recv, y_send, y_recv, f_send, f_recv, l_send, l_recv,
):
    s, t = lax.axis_index("seq"), lax.axis_index("tp")
    y, c = t // CORES, t % CORES
    rows = tp // CORES
    mate = y * CORES + 1 - c
    width = x_ref.shape[2]

    def block(group, shard):
        return out_ref.at[group, :, pl.ds(pl.multiple_of(shard * width, 128), width)]

    own = pltpu.make_async_copy(x_ref.at[s], block(s, t), local_sem.at[0])
    own.start()
    own_logits = pltpu.make_async_copy(part_ref, logits_ref.at[t], local_sem.at[1])
    own_logits.start()
    greet(seq, tp, s, t)
    order = interleaved(seq)
    sent = []
    spread = {}
    for off in order:
        spread[off] = remote(
            x_ref.at[flip(s, off)], block(s, t), a_send.at[off], a_recv.at[off], flip(s, off), t
        )
        spread[off].start()
    logit_copies = []
    for off in range(1, tp):
        copy = remote(
            part_ref, logits_ref.at[t], l_send.at[off], l_recv.at[off], s, (t + off) % tp
        )
        copy.start()
        logit_copies.append(copy)

    across = {}

    def relay(off):
        group = flip(s, off)
        for step in range(1, rows):
            across[off, step].wait_recv()
            origin = ((y + rows - step) % rows) * CORES + c
            copy = remote(
                block(group, origin), block(group, origin), f_send.at[step, off], f_recv.at[step, off], s, mate
            )
            copy.start()
            sent.append(copy)

    blocks = [0] + order
    for place, off in enumerate(blocks):
        group = flip(s, off)
        if off == 0:
            own.wait()
        else:
            spread[off].wait_recv()
        for step in range(1, rows):
            across[off, step] = remote(
                block(group, t), block(group, t), y_send.at[step, off], y_recv.at[step, off],
                s, ((y + step) % rows) * CORES + c,
            )
            across[off, step].start()
        copy = remote(block(group, t), block(group, t), d_send.at[off], d_recv.at[off], s, mate)
        copy.start()
        sent.append(copy)
        if place >= 2:
            relay(blocks[place - 2])
    for off in blocks[-2:]:
        relay(off)
    own_logits.wait()
    for copy in logit_copies:
        copy.wait()
    for copy in sent:
        copy.wait()
    for copy in across.values():
        copy.wait_send()
    for copy in spread.values():
        copy.wait_send()


def combine_kernel(
    seq, tp, p_ref, out_ref, mate_buf, half, across_buf, total,
    local_sem, a_send, a_recv, d_send, d_recv, y_send, y_recv,
):
    s, t = lax.axis_index("seq"), lax.axis_index("tp")
    y, c = t // CORES, t % CORES
    rows = tp // CORES
    mate = y * CORES + 1 - c
    width = out_ref.shape[2]

    def columns(shard):
        return pl.ds(pl.multiple_of(shard * width, 128), width)

    greet(seq, tp, s, t)
    order = list(range(seq // 2, seq)) + list(range(1, seq // 2)) + [0]
    pair = {}
    for off in order:
        group = flip(s, off)
        for step in list(range(1, rows)) + [0]:
            row = (y + step) % rows
            pair[off, step] = remote(
                p_ref.at[group, :, columns(row * CORES + 1 - c)], mate_buf.at[step, group],
                d_send.at[step, off], d_recv.at[step, off], s, mate,
            )
            pair[off, step].start()

    across = {}
    returned = {}

    def exchange(off):
        group = flip(s, off)
        for step in range(rows):
            row = (y + step) % rows
            pair[off, step].wait_recv()
            mine = p_ref[group, :, columns(row * CORES + c)].astype(jnp.float32)
            half[step, group] = (mine + mate_buf[step, group].astype(jnp.float32)).astype(jnp.bfloat16)
        for step in range(1, rows):
            across[off, step] = remote(
                half.at[step, group], across_buf.at[step, group], y_send.at[step, off], y_recv.at[step, off],
                s, ((y + step) % rows) * CORES + c,
            )
            across[off, step].start()

    def finish(off):
        group = flip(s, off)
        value = half[0, group].astype(jnp.float32)
        for step in range(1, rows):
            across[off, step].wait_recv()
            value = value + across_buf[step, group].astype(jnp.float32)
        total[group] = value.astype(jnp.bfloat16)
        if off == 0:
            copy = pltpu.make_async_copy(total.at[group], out_ref.at[s], local_sem)
        else:
            copy = remote(total.at[group], out_ref.at[s], a_send.at[off], a_recv.at[off], group, t)
        copy.start()
        returned[off] = copy

    for off in order:
        exchange(off)
    for off in order:
        finish(off)
    for copy in returned.values():
        copy.wait()
    for copy in across.values():
        copy.wait_send()
    for copy in pair.values():
        copy.wait_send()


def vmem(count):
    return [pl.BlockSpec(memory_space=pltpu.VMEM)] * count


def dispatch(seq, tp, outgoing, partial_logits):
    _, capacity, width = outgoing.shape
    rows = tp // CORES
    dma = pltpu.SemaphoreType.DMA
    return pl.pallas_call(
        functools.partial(dispatch_kernel, seq, tp),
        out_shape=(
            jax.ShapeDtypeStruct((seq, capacity, tp * width), jnp.bfloat16),
            jax.ShapeDtypeStruct((tp,) + partial_logits.shape, jnp.float32),
        ),
        in_specs=vmem(2),
        out_specs=tuple(vmem(2)),
        scratch_shapes=[
            dma((2,)), dma((seq,)), dma((seq,)), dma((seq,)), dma((seq,)),
            dma((rows, seq)), dma((rows, seq)), dma((rows, seq)), dma((rows, seq)),
            dma((tp,)), dma((tp,)),
        ],
        compiler_params=pltpu.CompilerParams(collective_id=0, has_side_effects=True),
        name="dispatch",
    )(outgoing, partial_logits)


def combine(seq, tp, partial_value):
    _, capacity, full = partial_value.shape
    width = full // tp
    rows = tp // CORES
    dma = pltpu.SemaphoreType.DMA
    return pl.pallas_call(
        functools.partial(combine_kernel, seq, tp),
        out_shape=jax.ShapeDtypeStruct((seq, capacity, width), jnp.bfloat16),
        in_specs=vmem(1),
        out_specs=vmem(1)[0],
        scratch_shapes=[
            pltpu.VMEM((rows, seq, capacity, width), jnp.bfloat16),
            pltpu.VMEM((rows, seq, capacity, width), jnp.bfloat16),
            pltpu.VMEM((rows, seq, capacity, width), jnp.bfloat16),
            pltpu.VMEM((seq, capacity, width), jnp.bfloat16),
            dma, dma((seq,)), dma((seq,)), dma((rows, seq)), dma((rows, seq)),
            dma((rows, seq)), dma((rows, seq)),
        ],
        compiler_params=pltpu.CompilerParams(collective_id=1, has_side_effects=True),
        name="combine",
    )(partial_value)


def per_device(seq, tp, tokens, router_weight, expert_ids, gate_weight, up_weight, down_weight):
    experts = router_weight.shape[1]
    halves = seq // experts
    tok_rows, top_count = expert_ids.shape
    flat_ids, slots = slot_numbers(expert_ids, experts)
    row_index = jnp.arange(seq * CAP, dtype=jnp.int32)
    row_expert = row_index // CAP // halves
    row_slot = row_index % CAP
    matches = (row_expert[:, None] == flat_ids[None, :]) & (row_slot[:, None] == slots[None, :])
    matches = matches.reshape(seq * CAP, tok_rows, top_count)
    select = jnp.any(matches, axis=2).astype(jnp.bfloat16)
    partial_logits = lax.dot_general(
        router_weight, tokens, (((0,), (1,)), ((), ())), preferred_element_type=jnp.float32
    )
    outgoing = jnp.dot(select, tokens, preferred_element_type=jnp.float32).astype(jnp.bfloat16)
    received, logit_parts = dispatch(seq, tp, outgoing.reshape(seq, CAP, -1), partial_logits)
    slot_rows = received.reshape(seq * CAP, -1)
    gate = jnp.dot(slot_rows, gate_weight[0], preferred_element_type=jnp.float32)
    up = jnp.dot(slot_rows, up_weight[0], preferred_element_type=jnp.float32)
    hidden = (jax.nn.silu(gate) * up).astype(jnp.bfloat16)
    partial_value = jnp.dot(hidden, down_weight[0], preferred_element_type=jnp.float32)
    returned = combine(seq, tp, partial_value.astype(jnp.bfloat16).reshape(seq, CAP, -1))

    logits = jnp.sum(logit_parts, axis=0).T
    chosen = expert_ids[:, :, None] == jnp.arange(experts, dtype=jnp.int32)[None, None, :]
    picked = jnp.sum(jnp.where(chosen, logits[:, None, :], 0.0), axis=2)
    gates = jax.nn.sigmoid(picked - picked[:, ::-1])
    weights = jnp.sum(jnp.where(matches, gates[None, :, :], 0.0), axis=2).T
    high = lax.reduce_precision(weights, 8, 7)
    low = weights - high
    summed = returned.reshape(seq * CAP, -1)
    mixed = jnp.dot(high.astype(jnp.bfloat16), summed, preferred_element_type=jnp.float32)
    mixed = mixed + jnp.dot(low.astype(jnp.bfloat16), summed, preferred_element_type=jnp.float32)
    return mixed.astype(jnp.bfloat16)


def solution(mesh):
    in_specs = (
        P("seq", "tp"),
        P("tp", None),
        P("seq", None),
        P("seq", None, "tp"),
        P("seq", None, "tp"),
        P("seq", "tp", None),
    )
    step = functools.partial(per_device, mesh.shape["seq"], mesh.shape["tp"])
    return jax.shard_map(
        step, mesh=mesh, in_specs=in_specs, out_specs=P("seq", "tp"), check_vma=False
    )
```
